32 devices in a mesh: gx: 4 (over y, core), gy: 4 (over z), gz: 2 (over x).
Axes of the slice: x: 2, y: 2, z: 4, core: 2. Of those that a mesh axis runs over, the one named last changes fastest.
Arguments:
- grads: bfloat16 [32, 4, 1, 8, 3584], P(('gx', 'gy', 'gz')), may hold values from -1196032 to 1196032
- counts: int32 [32], P(('gx', 'gy', 'gz')), may hold values from 1 to 4
- total_tokens: int32 [1], replicated, may hold values from 4000000 to 15999999
- master: float32 [1, 8, 3584], P(None, 'gy', ('gx', 'gz')), may hold values from -6 to 6
- moment1: float32 [1, 8, 3584], P(None, 'gy', ('gx', 'gz')), may hold values from -2 to 2
- moment2: float32 [1, 8, 3584], P(None, 'gy', ('gx', 'gz')), may hold values from 0.01 to 1
Outputs:
- params: bfloat16 [1, 8, 3584], replicated
- master_out: float32 [1, 8, 3584], P(None, 'gy', ('gx', 'gz'))
- moment1_out: float32 [1, 8, 3584], P(None, 'gy', ('gx', 'gz'))
- moment2_out: float32 [1, 8, 3584], P(None, 'gy', ('gx', 'gz'))
The draws below stay inside these ranges and needn't reach their ends.
All inputs are finite; a program needn't handle non-finite values.
Results may differ from the reference program's by a relative error of at most 0.0004.
Values may be sent and summed in bfloat16 or wider, within the bound.
A program may use at most 64 MiB of HBM per device.

```python
import math
import jax
import jax.numpy as jnp
from jax import lax

D = 3584
MICRO = 4
BUCKETS = 1
ROWS = 8
DEVICES = 32


def set_ends(result, stream_key, smallest, largest):
    extent = result.shape
    place = [jax.random.randint(jax.random.fold_in(stream_key, axis), (), 0, extent[axis]) for axis in range(len(extent))]
    result = result.at[tuple(place)].set(smallest)
    longest = extent.index(max(extent))
    place[longest] = (place[longest] + 1) % extent[longest]
    return result.at[tuple(place)].set(largest)


def raised(values, own_key, source, target, blocks, factor):
    owner, partner = [(jnp.arange(values.shape[dim]) // (values.shape[dim] // blocks)).reshape([-1 if axis == dim else 1 for axis in range(values.ndim)]) for dim in (source, target)]
    chosen = jax.random.permutation(own_key, blocks)[partner]
    strong = (owner == chosen) | (owner == (partner + blocks // 2) % blocks)
    return jnp.where(strong, factor * values, values)


def level_of(own_key, dims, split, smallest, top_value):
    def one(position, parts):
        heights = jax.random.uniform(jax.random.fold_in(jax.random.fold_in(own_key, 6), position), (parts,), jnp.float32, smallest / len(split), top_value / len(split))
        return jnp.repeat(jnp.exp(heights), dims[position] // parts).reshape((-1,) + (1,) * (len(dims) - position - 1))

    level = one(*split[0])
    for cut in split[1:]:
        level = level * one(*cut)
    return level


def centred(key, shape, scale, limit, cuts=(), held_as=jnp.bfloat16):
    result = scale * jax.random.normal(key, shape, jnp.float32)
    if cuts:
        result = result * level_of(key, shape, cuts, -0.22, 0.18)
    return jnp.clip(result, -limit, limit).astype(held_as)


def heavy_noise(stream_key, shape, deviation, reach, shards, heavy, held_as=jnp.bfloat16):
    entries = deviation * jax.random.normal(stream_key, shape, jnp.float32)
    if shards:
        entries = entries * level_of(stream_key, shape, shards, -0.22, 0.18)
    return jnp.clip(raised(entries, jax.random.fold_in(stream_key, 3), *heavy), -reach, reach).astype(held_as)


def setup_inputs(seed: int = 0) -> dict:
    keys = jax.random.split(jax.random.key(seed), 7)
    return {
        "grads": heavy_noise(keys[0], (DEVICES, MICRO, BUCKETS, ROWS, D), 200000.0, 1196032, ((0, 32),), (0, 3, 8, 2.0)),
        "counts": set_ends(jax.random.randint(keys[1], (DEVICES,), 1, 5), jax.random.fold_in(keys[1], 1), 1, 4).astype(jnp.int32),
        "total_tokens": jax.random.randint(keys[2], (1,), 4000000, 16000000).astype(jnp.int32),
        "master": centred(keys[3], (BUCKETS, ROWS, D), 1.0, 6.0, ((1, 4), (2, 8)), jnp.float32),
        "moment1": centred(keys[4], (BUCKETS, ROWS, D), 0.3, 2.0, ((1, 4), (2, 8)), jnp.float32),
        "moment2": jnp.clip(jnp.exp(math.log(1.0) - 4.6051702 * jax.random.uniform(keys[5], (BUCKETS, ROWS, D), jnp.float32) ** level_of(keys[5], (BUCKETS, ROWS, D), ((1, 4), (2, 8)), -0.2, 0.2)), 0.01, 1.0),
    }


def reference(grads, counts, total_tokens, master, moment1, moment2):
    slots = jnp.arange(MICRO, dtype=jnp.int32)

    def add_rank(carry, item):
        rank_grads, rank_count = item
        weights = (slots < rank_count).astype(jnp.float32)
        local = jnp.zeros(carry.shape, jnp.float32)
        for slot in range(MICRO):
            local = local + weights[slot] * rank_grads[slot].astype(jnp.float32)
        return (carry + local, None)
    start = jnp.zeros((BUCKETS, ROWS, D), jnp.float32)
    summed, unused = lax.scan(add_rank, start, (grads, counts))
    gradient = summed / total_tokens.astype(jnp.float32)[0]
    moment1_out = 0.9 * moment1 + 0.1 * gradient
    moment2_out = 0.95 * moment2 + 0.05 * gradient * gradient
    first_fix = 1.0 - 0.9 ** 10
    second_fix = 1.0 - 0.95 ** 10
    update = moment1_out / first_fix / (jnp.sqrt(moment2_out / second_fix) + 1e-08)
    master_out = master - 0.01 * (update + 0.1 * master)
    params = master_out.astype(jnp.bfloat16)
    return (params, master_out, moment1_out, moment2_out)
```

```python
import functools

import jax
import jax.numpy as jnp
from jax import lax
from jax.experimental import pallas as pl
from jax.experimental.pallas import tpu as pltpu
from jax.sharding import PartitionSpec as P

MESH = pl.DeviceIdType.MESH
LANES = 128


class Cut:
    def __init__(self, width, blocks):
        self.width, self.blocks = width, blocks
        self.own = width // blocks
        tiles = max(-(-(c + 1) * self.own // LANES) - c * self.own // LANES for c in range(blocks))
        self.window = tiles * LANES
        self.last = width // LANES - tiles
        self.offsets = sorted({self.offset(c) for c in range(blocks)})

    def tile(self, c):
        if isinstance(c, int):
            return min(c * self.own // LANES, self.last)
        return jnp.minimum(lax.div(c * self.own, LANES), self.last)

    def offset(self, c):
        return c * self.own - LANES * self.tile(c)

    def into(self, x, offset):
        rows = x.shape[0]
        result = None
        for o in self.offsets:
            parts = [jnp.zeros((rows, o), x.dtype)] if o else []
            parts.append(x)
            rest = self.window - o - self.own
            if rest:
                parts.append(jnp.zeros((rows, rest), x.dtype))
            moved = jnp.concatenate(parts, axis=1) if len(parts) > 1 else x
            result = moved if result is None else jnp.where(offset == o, moved, result)
        return result

    def out_of(self, x, offset):
        result = None
        for o in self.offsets:
            moved = x[:, o : o + self.own]
            result = moved if result is None else jnp.where(offset == o, moved, result)
        return result


def each_peer(sizes, me, visit):
    nx, ny, nz = sizes
    gx, gy, gz = me
    if nx * ny * nz <= 64:
        xs = [gx] + [lax.rem(gx + a, nx) for a in range(1, nx)]
        ys = [gy] + [lax.rem(gy + b, ny) for b in range(1, ny)]
        zs = [gz] + [lax.rem(gz + c, nz) for c in range(1, nz)]
        order = sorted(range(ny), key=lambda b: -min(b, ny - b))
        for b in order:
            for a in range(nx):
                for c in range(nz):
                    slot = (b * nx + a) * nz + c - 1
                    if slot >= 0:
                        visit(slot, (xs[a], ys[b], zs[c]))
    else:

        def step(k, carry):
            c = lax.rem(k, nz)
            a = lax.rem(lax.div(k, nz), nx)
            b = lax.div(k, nz * nx)
            visit(k - 1, (lax.rem(gx + a, nx), lax.rem(gy + b, ny), lax.rem(gz + c, nz)))
            return carry

        lax.fori_loop(1, nx * ny * nz, step, 0)


def kernel(
    sizes,
    cut,
    grads,
    counts,
    tokens,
    master,
    moment1,
    moment2,
    params_out,
    master_out,
    moment1_out,
    moment2_out,
    grad_buf,
    state_buf,
    count_buf,
    token_buf,
    stage,
    recv,
    shard,
    gathered,
    local_sem,
    rs_send,
    rs_recv,
    ag_send,
    ag_recv,
):
    nx, ny, nz = sizes
    n = nx * ny * nz
    gx, gy, gz = me = (lax.axis_index("gx"), lax.axis_index("gy"), lax.axis_index("gz"))
    rows = stage.shape[1]
    window = cut.window

    loads = [
        pltpu.make_async_copy(grads, grad_buf, local_sem.at[0]),
        pltpu.make_async_copy(counts, count_buf, local_sem.at[1]),
        pltpu.make_async_copy(tokens, token_buf, local_sem.at[2]),
        pltpu.make_async_copy(master, state_buf.at[0], local_sem.at[3]),
        pltpu.make_async_copy(moment1, state_buf.at[1], local_sem.at[4]),
        pltpu.make_async_copy(moment2, state_buf.at[2], local_sem.at[5]),
    ]
    for load in loads:
        load.start()

    barrier = pltpu.get_barrier_semaphore()
    each_peer(
        sizes,
        me,
        lambda slot, peer: pl.semaphore_signal(barrier, inc=1, device_id=peer, device_id_type=MESH),
    )

    loads[1].wait()
    loads[0].wait()
    count = count_buf[0]
    total = None
    for m in range(grad_buf.shape[0]):
        weight = jnp.where(m < count, jnp.float32(1.0), jnp.float32(0.0))
        term = weight * grad_buf[m].astype(jnp.float32)
        total = term if total is None else total + term
    for g in range(ny):
        stage[g] = total[g * rows : (g + 1) * rows]

    pl.semaphore_wait(barrier, n - 1)

    def send_sum(slot, peer):
        start = pl.multiple_of(LANES * cut.tile(peer[0] * nz + peer[2]), LANES)
        pltpu.make_async_remote_copy(
            src_ref=stage.at[peer[1], :, pl.ds(start, window)],
            dst_ref=recv.at[slot],
            send_sem=rs_send,
            recv_sem=rs_recv,
            device_id=peer,
            device_id_type=MESH,
        ).start()

    each_peer(sizes, me, send_sum)

    column = gx * nz + gz
    offset = cut.offset(column)
    for load in loads[2:]:
        load.wait()
    old_master = cut.into(state_buf[0], offset)
    old_moment1 = cut.into(state_buf[1], offset)
    old_moment2 = cut.into(state_buf[2], offset)
    scale = token_buf[0].astype(jnp.float32)
    start = pl.multiple_of(LANES * cut.tile(column), LANES)
    own = stage[gy, :, pl.ds(start, window)]

    pltpu.make_async_copy(recv, recv, rs_recv).wait()
    if n <= 64:
        terms = [own] + [recv[k] for k in range(n - 1)]
        while len(terms) > 1:
            terms = [a + b for a, b in zip(terms[::2], terms[1::2])] + terms[len(terms) - len(terms) % 2 :]
        summed = terms[0]
    else:
        summed = lax.fori_loop(0, n - 1, lambda k, s: s + recv[k], own)
    gradient = summed / scale
    new_moment1 = 0.9 * old_moment1 + 0.1 * gradient
    new_moment2 = 0.95 * old_moment2 + 0.05 * gradient * gradient
    first_fix = 1.0 - 0.9**10
    second_fix = 1.0 - 0.95**10
    update = new_moment1 / first_fix / (jnp.sqrt(new_moment2 / second_fix) + 1e-08)
    new_master = old_master - 0.01 * (update + 0.1 * old_master)
    new_params = new_master.astype(jnp.bfloat16)
    shard[...] = new_params

    mine = gy * (nx * nz) + column

    def send_params(slot, peer):
        pltpu.make_async_remote_copy(
            src_ref=shard,
            dst_ref=gathered.at[mine],
            send_sem=ag_send,
            recv_sem=ag_recv,
            device_id=peer,
            device_id_type=MESH,
        ).start()

    each_peer(sizes, me, send_params)

    gathered[mine] = new_params
    master_out[...] = cut.out_of(new_master, offset)
    moment1_out[...] = cut.out_of(new_moment1, offset)
    moment2_out[...] = cut.out_of(new_moment2, offset)
    pltpu.make_async_copy(recv, recv, rs_send).wait()
    others = gathered.at[pl.ds(0, n - 1)]
    pltpu.make_async_copy(others, others, ag_send).wait()
    pltpu.make_async_copy(others, others, ag_recv).wait()

    lane = lax.broadcasted_iota(jnp.int32, (rows, LANES), 1)
    for g in range(ny):
        tiles = []
        for t in range(cut.width // LANES):
            value = None
            for c in range(cut.blocks):
                first = c * cut.own - t * LANES
                if first + cut.own <= 0 or first >= LANES:
                    continue
                at = (t - cut.tile(c)) * LANES
                piece = gathered[g * cut.blocks + c, :, at : at + LANES]
                value = piece if value is None else jnp.where(lane >= first, piece, value)
            tiles.append(value)
        params_out[g * rows : (g + 1) * rows, :] = jnp.concatenate(tiles, axis=1)


def solution(mesh):
    sizes = tuple(mesh.shape[axis] for axis in ("gx", "gy", "gz"))
    nx, ny, nz = sizes
    n = nx * ny * nz

    def body(grads, counts, total_tokens, master, moment1, moment2):
        micro, _, all_rows, width = grads.shape[1:]
        rows, own = master.shape[1:]
        cut = Cut(width, nx * nz)
        anywhere = pl.BlockSpec(memory_space=pl.ANY)
        vmem = pl.BlockSpec(memory_space=pltpu.VMEM)
        part = jax.ShapeDtypeStruct((rows, own), jnp.float32)
        params, *state = pl.pallas_call(
            functools.partial(kernel, sizes, cut),
            out_shape=[jax.ShapeDtypeStruct((all_rows, width), jnp.bfloat16), part, part, part],
            in_specs=[anywhere] * 6,
            out_specs=[vmem] * 4,
            scratch_shapes=[
                pltpu.VMEM((micro, all_rows, width), jnp.bfloat16),
                pltpu.VMEM((3, rows, own), jnp.float32),
                pltpu.SMEM((1,), jnp.int32),
                pltpu.SMEM((1,), jnp.int32),
                pltpu.VMEM((ny, rows, width), jnp.float32),
                pltpu.VMEM((n - 1, rows, cut.window), jnp.float32),
                pltpu.VMEM((rows, cut.window), jnp.bfloat16),
                pltpu.VMEM((n, rows, cut.window), jnp.bfloat16),
                pltpu.SemaphoreType.DMA((6,)),
                pltpu.SemaphoreType.DMA,
                pltpu.SemaphoreType.DMA,
                pltpu.SemaphoreType.DMA,
                pltpu.SemaphoreType.DMA,
            ],
            compiler_params=pltpu.CompilerParams(collective_id=0, has_side_effects=True),
            name="step",
        )(
            grads.reshape(micro, all_rows, width),
            counts,
            total_tokens,
            master.reshape(rows, own),
            moment1.reshape(rows, own),
            moment2.reshape(rows, own),
        )
        return (params[None], *(array[None] for array in state))

    sharded = P(None, "gy", ("gx", "gz"))
    return jax.shard_map(
        body,
        mesh=mesh,
        in_specs=(P(("gx", "gy", "gz"), None, None, None, None), P(("gx", "gy", "gz")), P(), sharded, sharded, sharded),
        out_specs=(P(), sharded, sharded, sharded),
        check_vma=False,
    )
```

```python
import functools

import jax
import jax.numpy as jnp
from jax import lax
from jax.experimental import pallas as pl
from jax.experimental.pallas import tpu as pltpu
from jax.sharding import PartitionSpec as P

MESH = pl.DeviceIdType.MESH
LANES = 128


class Cut:
    def __init__(self, width, blocks):
        self.width, self.blocks = width, blocks
        self.own = width // blocks
        tiles = max(-(-(c + 1) * self.own // LANES) - c * self.own // LANES for c in range(blocks))
        self.window = tiles * LANES
        self.last = width // LANES - tiles
        self.offsets = sorted({self.offset(c) for c in range(blocks)})

    def tile(self, c):
        if isinstance(c, int):
            return min(c * self.own // LANES, self.last)
        return jnp.minimum(lax.div(c * self.own, LANES), self.last)

    def offset(self, c):
        return c * self.own - LANES * self.tile(c)

    def into(self, x, offset):
        rows = x.shape[0]
        result = None
        for o in self.offsets:
            parts = [jnp.zeros((rows, o), x.dtype)] if o else []
            parts.append(x)
            rest = self.window - o - self.own
            if rest:
                parts.append(jnp.zeros((rows, rest), x.dtype))
            moved = jnp.concatenate(parts, axis=1) if len(parts) > 1 else x
            result = moved if result is None else jnp.where(offset == o, moved, result)
        return result

    def out_of(self, x, offset):
        result = None
        for o in self.offsets:
            moved = x[:, o : o + self.own]
            result = moved if result is None else jnp.where(offset == o, moved, result)
        return result


def each_peer(sizes, me, visit):
    nx, ny, nz = sizes
    gx, gy, gz = me
    if nx * ny * nz <= 64:
        xs = [gx] + [lax.rem(gx + a, nx) for a in range(1, nx)]
        ys = [gy] + [lax.rem(gy + b, ny) for b in range(1, ny)]
        zs = [gz] + [lax.rem(gz + c, nz) for c in range(1, nz)]
        order = sorted(range(ny), key=lambda b: -min(b, ny - b))
        for b in order:
            for a in range(nx):
                for c in range(nz):
                    slot = (b * nx + a) * nz + c - 1
                    if slot >= 0:
                        visit(slot, (xs[a], ys[b], zs[c]))
    else:

        def step(k, carry):
            c = lax.rem(k, nz)
            a = lax.rem(lax.div(k, nz), nx)
            b = lax.div(k, nz * nx)
            visit(k - 1, (lax.rem(gx + a, nx), lax.rem(gy + b, ny), lax.rem(gz + c, nz)))
            return carry

        lax.fori_loop(1, nx * ny * nz, step, 0)


def kernel(
    sizes,
    cut,
    grads,
    counts,
    tokens,
    master,
    moment1,
    moment2,
    gathered,
    state,
    grad_buf,
    state_buf,
    stage,
    recv,
    shard,
    local_sem,
    rs_send,
    rs_recv,
    ag_send,
    ag_recv,
):
    nx, ny, nz = sizes
    n = nx * ny * nz
    gx, gy, gz = me = (lax.axis_index("gx"), lax.axis_index("gy"), lax.axis_index("gz"))
    rows = stage.shape[1]
    window = cut.window

    loads = [
        pltpu.make_async_copy(grads, grad_buf, local_sem.at[0]),
        pltpu.make_async_copy(master, state_buf.at[0], local_sem.at[3]),
        pltpu.make_async_copy(moment1, state_buf.at[1], local_sem.at[4]),
        pltpu.make_async_copy(moment2, state_buf.at[2], local_sem.at[5]),
    ]
    for load in loads:
        load.start()

    barrier = pltpu.get_barrier_semaphore()
    each_peer(
        sizes,
        me,
        lambda slot, peer: pl.semaphore_signal(barrier, inc=1, device_id=peer, device_id_type=MESH),
    )

    loads[0].wait()
    count = counts[0]
    total = None
    for m in range(grad_buf.shape[0]):
        weight = jnp.where(m < count, jnp.float32(1.0), jnp.float32(0.0))
        term = weight * grad_buf[m].astype(jnp.float32)
        total = term if total is None else total + term
    for g in range(ny):
        stage[g] = total[g * rows : (g + 1) * rows]

    pl.semaphore_wait(barrier, n - 1)

    def send_sum(slot, peer):
        start = pl.multiple_of(LANES * cut.tile(peer[0] * nz + peer[2]), LANES)
        pltpu.make_async_remote_copy(
            src_ref=stage.at[peer[1], :, pl.ds(start, window)],
            dst_ref=recv.at[slot],
            send_sem=rs_send,
            recv_sem=rs_recv,
            device_id=peer,
            device_id_type=MESH,
        ).start()

    each_peer(sizes, me, send_sum)

    column = gx * nz + gz
    offset = cut.offset(column)
    for load in loads[1:]:
        load.wait()
    old_master = cut.into(state_buf[0], offset)
    old_moment1 = cut.into(state_buf[1], offset)
    old_moment2 = cut.into(state_buf[2], offset)
    scale = tokens[0].astype(jnp.float32)
    start = pl.multiple_of(LANES * cut.tile(column), LANES)
    own = stage[gy, :, pl.ds(start, window)]

    pltpu.make_async_copy(recv, recv, rs_recv).wait()
    if n <= 64:
        terms = [own] + [recv[k] for k in range(n - 1)]
        while len(terms) > 1:
            terms = [a + b for a, b in zip(terms[::2], terms[1::2])] + terms[len(terms) - len(terms) % 2 :]
        summed = terms[0]
    else:
        summed = lax.fori_loop(0, n - 1, lambda k, s: s + recv[k], own)
    gradient = summed / scale
    new_moment1 = 0.9 * old_moment1 + 0.1 * gradient
    new_moment2 = 0.95 * old_moment2 + 0.05 * gradient * gradient
    first_fix = 1.0 - 0.9**10
    second_fix = 1.0 - 0.95**10
    update = new_moment1 / first_fix / (jnp.sqrt(new_moment2 / second_fix) + 1e-08)
    new_master = old_master - 0.01 * (update + 0.1 * old_master)
    new_params = new_master.astype(jnp.bfloat16)
    shard[...] = new_params

    mine = gy * (nx * nz) + column

    def send_params(slot, peer):
        pltpu.make_async_remote_copy(
            src_ref=shard,
            dst_ref=gathered.at[mine],
            send_sem=ag_send,
            recv_sem=ag_recv,
            device_id=peer,
            device_id_type=MESH,
        ).start()

    each_peer(sizes, me, send_params)

    gathered[mine] = new_params
    state[0] = new_master
    state[1] = new_moment1
    state[2] = new_moment2
    pltpu.make_async_copy(recv, recv, rs_send).wait()
    others = gathered.at[pl.ds(0, n - 1)]
    pltpu.make_async_copy(others, others, ag_send).wait()
    pltpu.make_async_copy(others, others, ag_recv).wait()


def finish(
    sizes, cut, gathered, state, params_out, master_out, moment1_out, moment2_out, params_buf, state_buf, sem
):
    nx, ny, nz = sizes
    rows = gathered.shape[1]
    offset = cut.offset(lax.axis_index("gx") * nz + lax.axis_index("gz"))
    copies = []
    for k, out in enumerate((master_out, moment1_out, moment2_out)):
        state_buf[k] = cut.out_of(state[k], offset)
        copies.append(pltpu.make_async_copy(state_buf.at[k], out, sem.at[k]))
        copies[-1].start()

    lane = lax.broadcasted_iota(jnp.int32, (rows, LANES), 1)
    for g in range(ny):
        tiles = []
        for t in range(cut.width // LANES):
            value = None
            for c in range(cut.blocks):
                first = c * cut.own - t * LANES
                if first + cut.own <= 0 or first >= LANES:
                    continue
                at = (t - cut.tile(c)) * LANES
                piece = gathered[g * cut.blocks + c, :, at : at + LANES]
                value = piece if value is None else jnp.where(lane >= first, piece, value)
            tiles.append(value)
        params_buf[g * rows : (g + 1) * rows, :] = jnp.concatenate(tiles, axis=1)
    copies.append(pltpu.make_async_copy(params_buf, params_out, sem.at[3]))
    copies[-1].start()
    for copy in copies:
        copy.wait()


def solution(mesh):
    sizes = tuple(mesh.shape[axis] for axis in ("gx", "gy", "gz"))
    nx, ny, nz = sizes
    n = nx * ny * nz

    def body(grads, counts, total_tokens, master, moment1, moment2):
        micro, _, all_rows, width = grads.shape[1:]
        rows, own = master.shape[1:]
        cut = Cut(width, nx * nz)
        hbm = pl.BlockSpec(memory_space=pltpu.HBM)
        vmem = pl.BlockSpec(memory_space=pltpu.VMEM)
        scalar = pl.BlockSpec(memory_space=pltpu.SMEM)
        part = jax.ShapeDtypeStruct((rows, own), jnp.float32)
        gathered, state = pl.pallas_call(
            functools.partial(kernel, sizes, cut),
            out_shape=[
                pltpu.VMEM((n, rows, cut.window), jnp.bfloat16),
                pltpu.VMEM((3, rows, cut.window), jnp.float32),
            ],
            in_specs=[hbm, scalar, scalar, hbm, hbm, hbm],
            out_specs=[vmem] * 2,
            scratch_shapes=[
                pltpu.VMEM((micro, all_rows, width), jnp.bfloat16),
                pltpu.VMEM((3, rows, own), jnp.float32),
                pltpu.VMEM((ny, rows, width), jnp.float32),
                pltpu.VMEM((n - 1, rows, cut.window), jnp.float32),
                pltpu.VMEM((rows, cut.window), jnp.bfloat16),
                pltpu.SemaphoreType.DMA((6,)),
                pltpu.SemaphoreType.DMA,
                pltpu.SemaphoreType.DMA,
                pltpu.SemaphoreType.DMA,
                pltpu.SemaphoreType.DMA,
            ],
            compiler_params=pltpu.CompilerParams(collective_id=0, has_side_effects=True),
            name="step",
        )(
            grads.reshape(micro, all_rows, width),
            counts,
            total_tokens,
            master.reshape(rows, own),
            moment1.reshape(rows, own),
            moment2.reshape(rows, own),
        )
        params, *parts = pl.pallas_call(
            functools.partial(finish, sizes, cut),
            out_shape=[jax.ShapeDtypeStruct((all_rows, width), jnp.bfloat16), part, part, part],
            in_specs=[vmem] * 2,
            out_specs=[hbm] * 4,
            scratch_shapes=[
                pltpu.VMEM((all_rows, width), jnp.bfloat16),
                pltpu.VMEM((3, rows, own), jnp.float32),
                pltpu.SemaphoreType.DMA((4,)),
            ],
            name="finish",
        )(
            pltpu.with_memory_space_constraint(gathered, pltpu.VMEM),
            pltpu.with_memory_space_constraint(state, pltpu.VMEM),
        )
        return (params[None], *(array[None] for array in parts))

    sharded = P(None, "gy", ("gx", "gz"))
    return jax.shard_map(
        body,
        mesh=mesh,
        in_specs=(P(("gx", "gy", "gz"), None, None, None, None), P(("gx", "gy", "gz")), P(), sharded, sharded, sharded),
        out_specs=(P(), sharded, sharded, sharded),
        check_vma=False,
    )
```

```python
import functools

import jax
import jax.numpy as jnp
from jax import lax
from jax.experimental import pallas as pl
from jax.experimental.pallas import tpu as pltpu
from jax.sharding import PartitionSpec as P

MESH = pl.DeviceIdType.MESH
LANES = 128


class Cut:
    def __init__(self, width, blocks):
        self.width, self.blocks = width, blocks
        self.own = width // blocks
        tiles = max(-(-(c + 1) * self.own // LANES) - c * self.own // LANES for c in range(blocks))
        self.window = tiles * LANES
        self.last = width // LANES - tiles
        self.offsets = sorted({self.offset(c) for c in range(blocks)})

    def tile(self, c):
        if isinstance(c, int):
            return min(c * self.own // LANES, self.last)
        return jnp.minimum(lax.div(c * self.own, LANES), self.last)

    def offset(self, c):
        return c * self.own - LANES * self.tile(c)

    def into(self, x, offset):
        rows = x.shape[0]
        result = None
        for o in self.offsets:
            parts = [jnp.zeros((rows, o), x.dtype)] if o else []
            parts.append(x)
            rest = self.window - o - self.own
            if rest:
                parts.append(jnp.zeros((rows, rest), x.dtype))
            moved = jnp.concatenate(parts, axis=1) if len(parts) > 1 else x
            result = moved if result is None else jnp.where(offset == o, moved, result)
        return result

    def out_of(self, x, offset):
        result = None
        for o in self.offsets:
            moved = x[:, o : o + self.own]
            result = moved if result is None else jnp.where(offset == o, moved, result)
        return result


def plane_peers(sizes, me):
    nx, ny, nz = sizes
    gx, gy, gz = me
    xs = [gx] + [lax.rem(gx + a, nx) for a in range(1, nx)]
    zs = [gz] + [lax.rem(gz + c, nz) for c in range(1, nz)]
    order = sorted(range(1, nx * nz), key=lambda k: (-min(k % nz, nz - k % nz), -min(k // nz, nx - k // nz)))
    return [(k - 1, (xs[k // nz], gy, zs[k % nz])) for k in order]


def line_peers(sizes, me):
    nx, ny, nz = sizes
    gx, gy, gz = me
    return [(gx, lax.rem(gy + b, ny), gz) for b in sorted(range(1, ny), key=lambda b: -min(b, ny - b))]


def send(src, dst, sems, k, peer):
    copy = pltpu.make_async_remote_copy(
        src_ref=src,
        dst_ref=dst,
        send_sem=sems.at[0, k],
        recv_sem=sems.at[1, k],
        device_id=peer,
        device_id_type=MESH,
    )
    copy.start()


def wait_all(ref, sem):
    pltpu.make_async_copy(ref, ref, sem).wait()


def tree_sum(terms):
    while len(terms) > 1:
        terms = [a + b for a, b in zip(terms[::2], terms[1::2])] + terms[len(terms) - len(terms) % 2 :]
    return terms[0]


def kernel(
    sizes,
    cut,
    grads,
    counts,
    tokens,
    master,
    moment1,
    moment2,
    gathered,
    state,
    grad_buf,
    lines,
    stage,
    recv,
    planes,
    shard,
    local_sem,
    sems,
):
    nx, ny, nz = sizes
    gx, gy, gz = me = (lax.axis_index("gx"), lax.axis_index("gy"), lax.axis_index("gz"))
    plane, line = plane_peers(sizes, me), line_peers(sizes, me)
    window = cut.window

    loads = [
        pltpu.make_async_copy(grads, grad_buf, local_sem.at[0]),
        pltpu.make_async_copy(master, lines.at[gy, 0], local_sem.at[1]),
        pltpu.make_async_copy(moment1, lines.at[gy, 1], local_sem.at[2]),
        pltpu.make_async_copy(moment2, lines.at[gy, 2], local_sem.at[3]),
    ]
    for load in loads:
        load.start()

    barrier = pltpu.get_barrier_semaphore()
    for peer in line + [peer for _, peer in plane]:
        pl.semaphore_signal(barrier, inc=1, device_id=peer, device_id_type=MESH)

    loads[0].wait()
    count = counts[0]
    total = None
    for m in range(grad_buf.shape[0]):
        weight = jnp.where(m < count, jnp.float32(1.0), jnp.float32(0.0))
        term = weight * grad_buf[m].astype(jnp.float32)
        total = term if total is None else total + term
    stage[...] = total

    pl.semaphore_wait(barrier, len(line) + len(plane))

    for slot, peer in plane:
        start = pl.multiple_of(LANES * cut.tile(peer[0] * nz + peer[2]), LANES)
        send(stage.at[:, pl.ds(start, window)], recv.at[slot], sems, 0, peer)
    for load in loads[1:]:
        load.wait()
    for peer in line:
        send(lines.at[gy], lines.at[gy], sems, 1, peer)

    column = gx * nz + gz
    offset = cut.offset(column)
    scale = tokens[0].astype(jnp.float32)
    start = pl.multiple_of(LANES * cut.tile(column), LANES)
    own = stage[:, pl.ds(start, window)]

    wait_all(recv, sems.at[1, 0])
    planes[gy] = tree_sum([own] + [recv[k] for k in range(len(plane))])
    for peer in line:
        send(planes.at[gy], planes.at[gy], sems, 2, peer)

    other_lines = lines.at[pl.ds(0, ny - 1)]
    wait_all(other_lines, sems.at[0, 1])
    wait_all(other_lines, sems.at[1, 1])
    old_master, old_moment1, old_moment2 = [
        cut.into(jnp.concatenate([lines[g, k] for g in range(ny)], axis=0), offset) for k in range(3)
    ]

    other_planes = planes.at[pl.ds(0, ny - 1)]
    wait_all(other_planes, sems.at[1, 2])
    summed = tree_sum([planes[g] for g in range(ny)])
    gradient = summed / scale
    new_moment1 = 0.9 * old_moment1 + 0.1 * gradient
    new_moment2 = 0.95 * old_moment2 + 0.05 * gradient * gradient
    first_fix = 1.0 - 0.9**10
    second_fix = 1.0 - 0.95**10
    update = new_moment1 / first_fix / (jnp.sqrt(new_moment2 / second_fix) + 1e-08)
    new_master = old_master - 0.01 * (update + 0.1 * old_master)
    new_params = new_master.astype(jnp.bfloat16)
    shard[...] = new_params
    for _, peer in plane:
        send(shard, gathered.at[column], sems, 3, peer)

    gathered[column] = new_params
    state[0] = new_master
    state[1] = new_moment1
    state[2] = new_moment2
    wait_all(recv, sems.at[0, 0])
    wait_all(other_planes, sems.at[0, 2])
    others = gathered.at[pl.ds(0, len(plane))]
    wait_all(others, sems.at[0, 3])
    wait_all(others, sems.at[1, 3])


def finish(
    sizes, cut, gathered, state, params_out, master_out, moment1_out, moment2_out, params_buf, state_buf, sem
):
    nx, ny, nz = sizes
    rows = state_buf.shape[1]
    gy = lax.axis_index("gy")
    offset = cut.offset(lax.axis_index("gx") * nz + lax.axis_index("gz"))
    copies = []
    for k, out in enumerate((master_out, moment1_out, moment2_out)):
        mine = state[k, 0:rows]
        for g in range(1, ny):
            mine = jnp.where(gy == g, state[k, g * rows : (g + 1) * rows], mine)
        state_buf[k] = cut.out_of(mine, offset)
        copies.append(pltpu.make_async_copy(state_buf.at[k], out, sem.at[k]))
        copies[-1].start()

    lane = lax.broadcasted_iota(jnp.int32, (params_buf.shape[0], LANES), 1)
    for t in range(cut.width // LANES):
        value = None
        for c in range(cut.blocks):
            first = c * cut.own - t * LANES
            if first + cut.own <= 0 or first >= LANES:
                continue
            at = (t - cut.tile(c)) * LANES
            piece = gathered[c, :, at : at + LANES]
            value = piece if value is None else jnp.where(lane >= first, piece, value)
        params_buf[:, t * LANES : (t + 1) * LANES] = value
    copies.append(pltpu.make_async_copy(params_buf, params_out, sem.at[3]))
    copies[-1].start()
    for copy in copies:
        copy.wait()


def solution(mesh):
    sizes = tuple(mesh.shape[axis] for axis in ("gx", "gy", "gz"))
    nx, ny, nz = sizes

    def body(grads, counts, total_tokens, master, moment1, moment2):
        micro, _, all_rows, width = grads.shape[1:]
        rows, own = master.shape[1:]
        cut = Cut(width, nx * nz)
        hbm = pl.BlockSpec(memory_space=pltpu.HBM)
        vmem = pl.BlockSpec(memory_space=pltpu.VMEM)
        scalar = pl.BlockSpec(memory_space=pltpu.SMEM)
        part = jax.ShapeDtypeStruct((rows, own), jnp.float32)
        gathered, state = pl.pallas_call(
            functools.partial(kernel, sizes, cut),
            out_shape=[
                pltpu.VMEM((nx * nz, all_rows, cut.window), jnp.bfloat16),
                pltpu.VMEM((3, all_rows, cut.window), jnp.float32),
            ],
            in_specs=[hbm, scalar, scalar, hbm, hbm, hbm],
            out_specs=[vmem] * 2,
            scratch_shapes=[
                pltpu.VMEM((micro, all_rows, width), jnp.bfloat16),
                pltpu.VMEM((ny, 3, rows, own), jnp.float32),
                pltpu.VMEM((all_rows, width), jnp.float32),
                pltpu.VMEM((nx * nz - 1, all_rows, cut.window), jnp.float32),
                pltpu.VMEM((ny, all_rows, cut.window), jnp.float32),
                pltpu.VMEM((all_rows, cut.window), jnp.bfloat16),
                pltpu.SemaphoreType.DMA((4,)),
                pltpu.SemaphoreType.DMA((2, 4)),
            ],
            compiler_params=pltpu.CompilerParams(collective_id=0, has_side_effects=True),
            name="step",
        )(
            grads.reshape(micro, all_rows, width),
            counts,
            total_tokens,
            master.reshape(rows, own),
            moment1.reshape(rows, own),
            moment2.reshape(rows, own),
        )
        params, *parts = pl.pallas_call(
            functools.partial(finish, sizes, cut),
            out_shape=[jax.ShapeDtypeStruct((all_rows, width), jnp.bfloat16), part, part, part],
            in_specs=[vmem] * 2,
            out_specs=[hbm] * 4,
            scratch_shapes=[
                pltpu.VMEM((all_rows, width), jnp.bfloat16),
                pltpu.VMEM((3, rows, own), jnp.float32),
                pltpu.SemaphoreType.DMA((4,)),
            ],
            name="finish",
        )(
            pltpu.with_memory_space_constraint(gathered, pltpu.VMEM),
            pltpu.with_memory_space_constraint(state, pltpu.VMEM),
        )
        return (params[None], *(array[None] for array in parts))

    sharded = P(None, "gy", ("gx", "gz"))
    return jax.shard_map(
        body,
        mesh=mesh,
        in_specs=(P(("gx", "gy", "gz"), None, None, None, None), P(("gx", "gy", "gz")), P(), sharded, sharded, sharded),
        out_specs=(P(), sharded, sharded, sharded),
        check_vma=False,
    )
```
